32 devices in a mesh: rep: 4 (over y, x), exp: 8 (over z, core).
Axes of the slice: x: 2, y: 2, z: 4, core: 2. Of those that a mesh axis runs over, the one named last changes fastest.
Arguments:
- tokens: bfloat16 [4096, 3584], P(('rep', 'exp')), parts along dimension 0, may hold values from -6 to 6
- expert_ids: int32 [4096, 4], P(('rep', 'exp')), parts along dimension 0, may hold values from 0 to 7, all different within a row; in each aligned block of 128 rows (0 to 127, 128 to 255, ...) at most 96 rows name the same one
- gate_probs: float32 [4096, 4], P(('rep', 'exp')), parts along dimension 0, may hold values from 0.1 to 1
- placed: int32 [8], replicated, may hold values from 0 to 7, each once
- w_gate: bfloat16 [8, 3584, 1024], P('exp'), may hold values from -0.09375 to 0.09375
- w_up: bfloat16 [8, 3584, 1024], P('exp'), may hold values from -0.09375 to 0.09375
- w_down: bfloat16 [8, 1024, 3584], P('exp'), may hold values from -0.1875 to 0.1875
Outputs:
- mixed: bfloat16 [4096, 3584], P(('rep', 'exp')), parts along dimension 0
The draws below stay inside these ranges and needn't reach their ends.
There are 4 independent parts, one for each index of `rep`. The reference program is written for one: setup_inputs(seed, part) draws one part's arguments, and reference() takes and returns one part's arrays. A program takes and returns all parts, laid end to end along the dimension named above; an argument that names none is the same for every part. Nothing has to cross between parts.
Inputs may be any that keep to these rules, and one draw needn't show every extreme that they name: `expert_ids`: each row names 4 different experts. In the rows of one device no expert is named more than 96 times, a bound that some block reaches. `placed`: each expert once.
All inputs are finite; a program needn't handle non-finite values.
Results may differ from the reference program's by a relative error of at most 0.008.
Values may be sent and summed in bfloat16 or wider, within the bound.
No kernel may reach another device: no remote copies, remote signals or barrier semaphores. Data moves between devices by JAX's collectives and lax.ppermute only.
A program may use at most 192 MiB of HBM per device.

```python
import math
import jax
import jax.numpy as jnp
import numpy as np
from jax import lax

D = 3584
HID = 1024
TOPK = 4
TOK_DEV = 128
EXPERTS = 8
TOKENS = 1024
CAP = 96
N_EXP = 8


def steps_of(key, extent, split, smallest, top_value):
    level, own = 1.0, jax.random.fold_in(key, 6)
    for dim, parts in split:
        draws = jnp.exp(jax.random.uniform(jax.random.fold_in(own, dim), (parts,), jnp.float32, smallest / len(split), top_value / len(split)))
        level = level * jnp.repeat(draws, extent[dim] // parts).reshape([-1 if axis == dim else 1 for axis in range(len(extent))])
    return level


def assign_block(own_key, own, number, rows, count, top, most, lean):
    order = jax.random.permutation(own_key, count)
    crowded, common = load_shares(count, rows * top, most, lean, True), load_shares(count, rows * top, most, lean, False)
    places = jnp.arange(count)

    def named(tallies, offset_by):
        used = int((tallies > 0).sum())
        fixed = max(1, used // 4)
        passed = fixed + (places - fixed + offset_by * (used - fixed)) % max(1, count - fixed)
        return jnp.zeros((count,), jnp.int32).at[order[jnp.where(places < fixed, places, passed)]].set(jnp.asarray(tallies, jnp.int32))

    tallies = jnp.where(number % 4 == 0, named(crowded, number // 4), named(common, number - number // 4 - 1))
    mixed = jax.random.permutation(jax.random.fold_in(own, 3), count)
    giver, receiver = mixed[0:count // 2 * 2:2], mixed[1:count // 2 * 2:2]
    slack = jnp.minimum(tallies[giver] - 1, most - tallies[receiver]) // 2
    slack = jnp.where((giver == order[0]) | (receiver == order[0]) | (tallies[receiver] == 0), 0, jnp.maximum(slack, 0))
    passed = jax.random.randint(jax.random.fold_in(own, 4), (count // 2,), 0, 1 << 20) % (slack + 1)
    tallies = tallies.at[giver].add(-passed).at[receiver].add(passed)
    members = jnp.searchsorted(jnp.cumsum(tallies), jnp.arange(rows * top), side="right").astype(jnp.int32)
    listing = members.reshape(top, rows).T
    listing = listing[jax.random.permutation(jax.random.fold_in(own, 1), rows)]
    offset_by = jax.random.randint(jax.random.fold_in(own, 2), (rows, 1), 0, top)
    return jnp.take_along_axis(listing, (jnp.arange(top)[None, :] + offset_by) % top, axis=1)


def load_shares(count, total, reach, slope, full):
    loads = [(1 << 20) // math.isqrt(rank ** slope) + 1 for rank in range(1, count + 1)]
    largest = reach if full else min(reach, max(-(-total // count), total * loads[0] // sum(loads)))
    least = 1 if total - largest >= count - 1 else 0
    given, surplus = [largest] + [least] * (count - 1), total - largest - least * (count - 1)
    while surplus > 0:
        movable = [i for i in range(1, count) if given[i] < largest] or [i for i in range(1, count) if given[i] < reach]
        pool, remaining = sum([loads[i] for i in movable]), surplus
        for i in movable:
            extra = min(reach - given[i], max(1, remaining * loads[i] // pool), surplus)
            given[i] = given[i] + extra
            surplus = surplus - extra
    return np.array(given)


def normal_values(own_key, extent, deviation, limit, cuts=(), kind=jnp.bfloat16):
    values = deviation * jax.random.normal(own_key, extent, jnp.float32)
    if cuts:
        values = values * steps_of(own_key, extent, cuts, -0.22, 0.18)
    return jnp.clip(values, -limit, limit).astype(kind)


def setup_inputs(seed: int = 0, part: int = 0) -> dict:
    keys = jax.random.split(jax.random.key(seed), 8)
    part_splits = jax.random.split(jax.random.fold_in(keys[7], part), 8)
    tokens = normal_values(part_splits[0], (TOKENS, D), 1.0, 6.0, ((0, 8),))
    expert_ids_keys = jax.random.split(jax.random.fold_in(part_splits[1], 1), TOKENS // TOK_DEV)
    expert_ids_turns = jax.random.permutation(jax.random.fold_in(part_splits[1], 3), TOKENS // TOK_DEV)
    expert_ids = jax.vmap(lambda own, number: assign_block(jax.random.fold_in(part_splits[1], 2), own, number, TOK_DEV, EXPERTS, TOPK, CAP, 2))(expert_ids_keys, expert_ids_turns).reshape((TOKENS, TOPK))
    gate_probs = jnp.clip(0.1 + 0.9 * jax.random.uniform(part_splits[2], (TOKENS, TOPK), jnp.float32) ** steps_of(part_splits[2], (TOKENS, TOPK), ((0, 8),), -0.2, 0.2), 0.1, 1.0)
    placed = jax.random.permutation(keys[3], EXPERTS).astype(jnp.int32)
    w_gate = normal_values(keys[4], (EXPERTS, D, HID), D ** -0.5, 0.09375, ((0, 8),))
    w_up = normal_values(keys[5], (EXPERTS, D, HID), D ** -0.5, 0.09375, ((0, 8),))
    w_down = normal_values(keys[6], (EXPERTS, HID, D), HID ** -0.5, 0.1875, ((0, 8),))
    return dict(tokens=tokens, expert_ids=expert_ids, gate_probs=gate_probs, placed=placed, w_gate=w_gate, w_up=w_up, w_down=w_down)


def reference(tokens, expert_ids, gate_probs, placed, w_gate, w_up, w_down):
    flat_ids = expert_ids.reshape(-1)
    flat_probs = gate_probs.reshape(-1)
    owner = (jnp.arange(TOKENS * TOPK, dtype=jnp.int32) // TOPK).astype(jnp.int32)
    room = N_EXP * CAP

    def one_expert(total, inputs):
        expert, gate_w, up_w, down_w = inputs
        match = flat_ids == expert
        rank = jnp.cumsum(match.astype(jnp.int32)) - 1
        where_to = jnp.where(match, rank, room).astype(jnp.int32)
        slot_tok = jnp.full((room,), TOKENS, jnp.int32).at[where_to].set(owner, mode="drop")
        slot_prob = jnp.zeros((room,), jnp.float32).at[where_to].set(flat_probs, mode="drop")
        rows = jnp.take(tokens, slot_tok, axis=0, mode="fill", fill_value=0)
        gate = jnp.dot(rows, gate_w, preferred_element_type=jnp.float32)
        up = jnp.dot(rows, up_w, preferred_element_type=jnp.float32)
        hidden = (jax.nn.silu(gate) * up).astype(jnp.bfloat16)
        result = jnp.dot(hidden, down_w, preferred_element_type=jnp.float32).astype(jnp.bfloat16)
        weighted = slot_prob[:, None] * result.astype(jnp.float32)
        total = total.at[slot_tok].add(weighted, mode="drop")
        return total, None

    start = jnp.zeros((TOKENS, D), jnp.float32)
    total, _ = lax.scan(one_expert, start, (placed, w_gate, w_up, w_down))
    return total.astype(jnp.bfloat16)
```

```python
import jax
import jax.numpy as jnp
from jax import lax
from jax.sharding import PartitionSpec as P

TOK_DEV = 128
CORES = 2
LINE = 4
LANES = 128


def expert_rows(rows, gate_w, up_w, down_w):
    gate = jnp.dot(rows, gate_w, preferred_element_type=jnp.float32)
    up = jnp.dot(rows, up_w, preferred_element_type=jnp.float32)
    hidden = (jax.nn.silu(gate) * up).astype(jnp.bfloat16)
    return jnp.dot(hidden, down_w, preferred_element_type=jnp.float32).astype(jnp.bfloat16)


def run_expert(received, gate_w, up_w, down_w):
    sources, room, width = received.shape
    total_rows = sources * room
    flat = received.reshape(total_rows, width)
    result = expert_rows(flat, gate_w, up_w, down_w)
    return result.reshape(sources, room, width)


def sparse_body(tokens, expert_ids, gate_probs, placed, w_gate, w_up, w_down):
    tok_rows, width = tokens.shape
    picks = expert_ids.shape[1]
    devices = lax.axis_size("exp")
    average = tok_rows * picks // devices
    room = average + max(1, tok_rows * picks // (2 * devices))
    here = lax.axis_index("exp")
    mine = placed[here]
    gate_w, up_w, down_w = (w_gate[0], w_up[0], w_down[0])
    numbers = jnp.arange(devices, dtype=jnp.int32)
    home = jnp.sum(jnp.where(placed[None, :] == numbers[:, None], numbers[None, :], 0), axis=1)
    flat_ids = expert_ids.reshape(-1)
    target_dev = jnp.take(home, flat_ids)
    one_hot = (target_dev[:, None] == numbers[None, :]).astype(jnp.int32)
    rank = jnp.sum((jnp.cumsum(one_hot, axis=0) - 1) * one_hot, axis=1)
    slot_index = target_dev * room + rank
    rows_x = lax.all_gather(tokens, "exp", axis=0, tiled=True)
    rows_ids = lax.all_gather(expert_ids.astype(jnp.bfloat16), "exp", axis=0, tiled=True)
    shards = rows_x.shape[0] // TOK_DEV
    match = rows_ids.astype(jnp.int32).reshape(shards, TOK_DEV * picks) == mine
    order = jnp.cumsum(match.astype(jnp.int32), axis=1) - 1
    spot = jnp.where(match, order, room)
    within = jnp.broadcast_to(
        (jnp.arange(TOK_DEV * picks, dtype=jnp.int32) // picks)[None, :], (shards, TOK_DEV * picks)
    )
    shard_num = jnp.broadcast_to(
        jnp.arange(shards, dtype=jnp.int32)[:, None], (shards, TOK_DEV * picks)
    )
    slot_tok = (
        jnp.full((shards, room), TOK_DEV, jnp.int32).at[shard_num, spot].set(within, mode="drop")
    )
    global_row = jnp.where(
        slot_tok < TOK_DEV,
        jnp.arange(shards, dtype=jnp.int32)[:, None] * TOK_DEV + slot_tok,
        shards * TOK_DEV,
    )
    got = jnp.take(rows_x, global_row.reshape(-1), axis=0, mode="fill", fill_value=0)
    got = got.reshape(shards, room, width)
    counts = jnp.sum(match, axis=1)
    received, counts = (got, counts)
    produced = run_expert(received, gate_w, up_w, down_w)
    returned = lax.all_to_all(produced, "exp", split_axis=0, concat_axis=0, tiled=True)
    picked = jnp.take(returned.reshape(devices * room, width), slot_index, axis=0)
    picked = picked.reshape(tok_rows, picks, width)
    mixed = jnp.einsum("tk,tkd->td", gate_probs, picked.astype(jnp.float32))
    return mixed.astype(jnp.bfloat16)


def line_body(tokens, expert_ids, gate_probs, placed, w_gate, w_up, w_down):
    tok_rows, width = tokens.shape
    devices = lax.axis_size("exp")
    here = lax.axis_index("exp")
    chip = here // CORES
    chips = devices // CORES
    last = chips - 1
    outer = (chip == 0) | (chip == last)
    half = tok_rows // 2

    def spread(pairs):
        return [(CORES * a + c, CORES * b + c) for a, b in pairs for c in range(CORES)]

    stay = [(0, 0), (last, last)]
    pair = spread([(0, 1), (1, 0), (last - 1, last), (last, last - 1)])
    middle = spread([(1, 2), (2, 1)] + stay)
    twins = [(i, i ^ 1) for i in range(devices)]

    def send(value, perm):
        return lax.ppermute(value, "exp", perm)

    weight = jnp.sum(
        jnp.where(expert_ids[:, :, None] == placed[None, None, :], gate_probs[:, :, None], 0.0), axis=1
    )
    high = lax.reduce_precision(weight, 8, 7)
    low = weight - high
    packed = jnp.concatenate([high, low, jnp.zeros((tok_rows, LANES - 2 * devices), jnp.float32)], axis=1)
    rows = jnp.concatenate([tokens, packed.astype(jnp.bfloat16)], axis=1)
    own_a, own_b = rows[:half], rows[half:]

    gate_w, up_w, down_w = w_gate[0], w_up[0], w_down[0]
    lane = jnp.arange(LANES)
    mine = (lane == here) | (lane == here + devices)

    def run(block):
        other = send(block, twins)
        both = jnp.concatenate([block, other], axis=0)
        x = both[:, :width]
        scale = jnp.sum(jnp.where(mine[None, :], both[:, width:].astype(jnp.float32), 0.0), axis=1)
        gate = jnp.dot(x, gate_w, preferred_element_type=jnp.float32)
        up = jnp.dot(x, up_w, preferred_element_type=jnp.float32)
        hidden = (jax.nn.silu(gate) * up).astype(jnp.bfloat16)
        result = jnp.dot(hidden, down_w, preferred_element_type=jnp.float32) * scale[:, None]
        n = block.shape[0]
        back = send(result[n:].astype(jnp.bfloat16), twins)
        return result[:n] + back.astype(jnp.float32)

    def pick(a, b):
        return jnp.where(outer, a, b)

    def low_bits(v):
        return v.astype(jnp.bfloat16)

    def wide(v):
        return v.astype(jnp.float32)

    def fit(v):
        return jnp.concatenate([low_bits(v), jnp.zeros((v.shape[0], LANES), jnp.bfloat16)], axis=1)

    def cut(v):
        return wide(v[:, :width])

    g0 = send(own_a, pair)
    m0 = send(own_a, middle)
    g1 = send(pick(own_b, m0), pair)
    m1 = send(g0, middle)
    p_near_a = run(g0)
    m2 = send(g1, middle)
    g2 = send(pick(fit(p_near_a), m1), pair)
    p_mid_a = run(pick(g1, m0))
    m3 = send(own_b, middle)
    g3 = send(pick(fit(p_mid_a), m2), pair)
    p_far_a = run(pick(g2, m1))
    m4 = send(low_bits(p_mid_a + cut(g3)), middle)
    g4 = send(pick(fit(p_far_a), m3), pair)
    p_far_b = run(pick(g3, m2))
    m5 = send(low_bits(p_far_a + cut(g4)), middle)
    g5 = send(pick(fit(p_far_b), own_b), pair)
    p_mid_b = run(pick(g4, m3))
    m6 = send(low_bits(p_far_b + cut(g5)), middle)
    g6 = send(low_bits(pick(p_mid_b, p_near_a + wide(m5))), pair)
    p_near_b = run(pick(g5, g1))
    m7 = send(low_bits(p_mid_b + wide(g6)), middle)
    g7 = send(low_bits(pick(p_near_b, p_near_b + wide(m6))), pair)
    own = run(rows)
    top = own[:half] + pick(wide(g6), cut(g2) + wide(m4))
    bottom = own[half:] + pick(wide(g7), wide(g7) + wide(m7))
    return jnp.concatenate([low_bits(top), low_bits(bottom)], axis=0)


def body(tokens, *rest):
    if lax.axis_size("exp") == CORES * LINE:
        return line_body(tokens, *rest)
    return sparse_body(tokens, *rest)


def solution(mesh):
    return jax.shard_map(
        body,
        mesh=mesh,
        in_specs=(
            P(("rep", "exp"), None),
            P(("rep", "exp"), None),
            P(("rep", "exp"), None),
            P(),
            P("exp", None, None),
            P("exp", None, None),
            P("exp", None, None),
        ),
        out_specs=P(("rep", "exp"), None),
        check_vma=False,
    )
```

```python
import functools
import jax
import jax.numpy as jnp
from jax import lax
from jax.experimental import pallas as pl
from jax.experimental.pallas import tpu as pltpu
from jax.sharding import PartitionSpec as P


TOK_DEV = 128
CORES = 2
LINE = 4
LANES = 128


def expert_rows(rows, gate_w, up_w, down_w):
    gate = jnp.dot(rows, gate_w, preferred_element_type=jnp.float32)
    up = jnp.dot(rows, up_w, preferred_element_type=jnp.float32)
    hidden = (jax.nn.silu(gate) * up).astype(jnp.bfloat16)
    return jnp.dot(hidden, down_w, preferred_element_type=jnp.float32).astype(jnp.bfloat16)


def run_expert(received, gate_w, up_w, down_w):
    sources, room, width = received.shape
    total_rows = sources * room
    flat = received.reshape(total_rows, width)
    result = expert_rows(flat, gate_w, up_w, down_w)
    return result.reshape(sources, room, width)


def sparse_body(tokens, expert_ids, gate_probs, placed, w_gate, w_up, w_down):
    tok_rows, width = tokens.shape
    picks = expert_ids.shape[1]
    devices = lax.axis_size("exp")
    average = tok_rows * picks // devices
    room = average + max(1, tok_rows * picks // (2 * devices))
    here = lax.axis_index("exp")
    mine = placed[here]
    gate_w, up_w, down_w = (w_gate[0], w_up[0], w_down[0])
    numbers = jnp.arange(devices, dtype=jnp.int32)
    home = jnp.sum(jnp.where(placed[None, :] == numbers[:, None], numbers[None, :], 0), axis=1)
    flat_ids = expert_ids.reshape(-1)
    target_dev = jnp.take(home, flat_ids)
    one_hot = (target_dev[:, None] == numbers[None, :]).astype(jnp.int32)
    rank = jnp.sum((jnp.cumsum(one_hot, axis=0) - 1) * one_hot, axis=1)
    slot_index = target_dev * room + rank
    rows_x = lax.all_gather(tokens, "exp", axis=0, tiled=True)
    rows_ids = lax.all_gather(expert_ids.astype(jnp.bfloat16), "exp", axis=0, tiled=True)
    shards = rows_x.shape[0] // TOK_DEV
    match = rows_ids.astype(jnp.int32).reshape(shards, TOK_DEV * picks) == mine
    order = jnp.cumsum(match.astype(jnp.int32), axis=1) - 1
    spot = jnp.where(match, order, room)
    within = jnp.broadcast_to(
        (jnp.arange(TOK_DEV * picks, dtype=jnp.int32) // picks)[None, :], (shards, TOK_DEV * picks)
    )
    shard_num = jnp.broadcast_to(
        jnp.arange(shards, dtype=jnp.int32)[:, None], (shards, TOK_DEV * picks)
    )
    slot_tok = (
        jnp.full((shards, room), TOK_DEV, jnp.int32).at[shard_num, spot].set(within, mode="drop")
    )
    global_row = jnp.where(
        slot_tok < TOK_DEV,
        jnp.arange(shards, dtype=jnp.int32)[:, None] * TOK_DEV + slot_tok,
        shards * TOK_DEV,
    )
    got = jnp.take(rows_x, global_row.reshape(-1), axis=0, mode="fill", fill_value=0)
    got = got.reshape(shards, room, width)
    counts = jnp.sum(match, axis=1)
    received = got
    produced = run_expert(received, gate_w, up_w, down_w)
    returned = lax.all_to_all(produced, "exp", split_axis=0, concat_axis=0, tiled=True)
    picked = jnp.take(returned.reshape(devices * room, width), slot_index, axis=0)
    picked = picked.reshape(tok_rows, picks, width)
    mixed = jnp.einsum("tk,tkd->td", gate_probs, picked.astype(jnp.float32))
    return mixed.astype(jnp.bfloat16)


def run_kernel(width, devices, spot, block, twin, gate_w, up_w, down_w, own, other, rows):
    half = own.shape[0]
    rows[:half] = block[...]
    rows[half:] = twin[...]
    lane = lax.broadcasted_iota(jnp.int32, (2 * half, LANES), 1)
    mine = (lane == spot[0]) | (lane == spot[0] + devices)
    weights = rows[:, width:].astype(jnp.float32)
    scale = jnp.sum(jnp.where(mine, weights, 0.0), axis=1, keepdims=True)
    x = rows[:, :width]
    gate = jnp.dot(x, gate_w[...], preferred_element_type=jnp.float32)
    up = jnp.dot(x, up_w[...], preferred_element_type=jnp.float32)
    hidden = (gate / (1.0 + jnp.exp(-gate)) * up).astype(jnp.bfloat16)
    result = jnp.dot(hidden, down_w[...], preferred_element_type=jnp.float32) * scale
    own[...] = result[:half]
    other[...] = result[half:].astype(jnp.bfloat16)


def at_end(spot):
    return (spot[0] < CORES) | (spot[0] >= CORES * (LINE - 1))


def load_kernel(source, after, held, sem):
    copy = pltpu.make_async_copy(source.at[0], held, sem)
    copy.start()
    copy.wait()


def prepare_kernel(devices, placed_hbm, tokens_hbm, ids_hbm, probs_hbm, *refs):
    outs, (placed, tokens, ids, probs, sems) = refs[:5], refs[5:]
    rows, width = tokens.shape
    copies = [
        pltpu.make_async_copy(src, dst, sems.at[n])
        for n, (src, dst) in enumerate(
            ((placed_hbm, placed), (ids_hbm, ids), (probs_hbm, probs), (tokens_hbm, tokens))
        )
    ]
    for copy in copies:
        copy.start()
    for copy in copies[:3]:
        copy.wait()
    slot = lax.broadcasted_iota(jnp.int32, (LANES, rows), 0)
    weight = jnp.zeros((LANES, rows), jnp.float32)
    for s in range(devices):
        total = jnp.zeros((1, rows), jnp.float32)
        for k in range(ids.shape[0]):
            total += jnp.where(ids[k : k + 1, :] == placed[s], probs[k : k + 1, :], 0.0)
        high = total.astype(jnp.bfloat16).astype(jnp.float32)
        weight = jnp.where(slot == s, high, jnp.where(slot == s + devices, total - high, weight))
    packed = weight.T.astype(jnp.bfloat16)
    copies[3].wait()
    start = 0
    for out in outs[:-1]:
        size = out.shape[0]
        out[:, :width] = tokens[start : start + size, :]
        out[:, width:] = packed[start : start + size, :]
        start += size
    outs[-1][:, :width] = tokens[...]
    outs[-1][:, width:] = packed


def gate_kernel(before, out):
    out[...] = before[...]


def join_kernel(spot, outer_x, outer_y, inner_x, inner_y, gate, out):
    part = outer_x.shape[0]

    @pl.when(at_end(spot))
    def _():
        out[:part] = outer_x[...]
        out[part:] = outer_y[...]

    @pl.when(jnp.logical_not(at_end(spot)))
    def _():
        out[:part] = inner_x[...]
        out[part:] = inner_y[...]


def over_kernel(start, spot, own, back, passed, out):
    part, width = out.shape[0], own.shape[1]

    @pl.when(at_end(spot))
    def _():
        total = own[start : start + part] + back[start : start + part].astype(jnp.float32)
        out[:, :width] = total.astype(out.dtype)
        out[:, width:] = jnp.zeros((part, out.shape[1] - width), out.dtype)

    @pl.when(jnp.logical_not(at_end(spot)))
    def _():
        out[...] = passed[...]


def pass_kernel(spot, mine, passed, out):
    @pl.when(at_end(spot))
    def _():
        out[...] = mine[...]

    @pl.when(jnp.logical_not(at_end(spot)))
    def _():
        out[...] = passed[...]


def add_kernel(start, spot, own, back, other, out):
    part, width = out.shape
    total = own[start : start + part] + back[start : start + part].astype(jnp.float32)
    out[...] = (total + other[:, :width].astype(jnp.float32)).astype(out.dtype)


def ends_kernel(start, spot, outer_own, outer_back, inner_own, inner_back, other, out):
    part = out.shape[0]

    @pl.when(at_end(spot))
    def _():
        total = outer_own[start : start + part] + outer_back[start : start + part].astype(jnp.float32)
        out[...] = total.astype(out.dtype)

    @pl.when(jnp.logical_not(at_end(spot)))
    def _():
        total = inner_own[start : start + part] + inner_back[start : start + part].astype(jnp.float32)
        out[...] = (total + other[...].astype(jnp.float32)).astype(out.dtype)


def finish_kernel(spot, own, back, *refs):
    out = refs[-1]
    part, width = refs[0].shape
    for n in range(4):
        sums, near, far = refs[3 * n : 3 * n + 3]
        rows = slice(n * part, (n + 1) * part)
        total = own[rows] + back[rows].astype(jnp.float32)

        @pl.when(at_end(spot))
        def _():
            out[rows] = (total + sums[...].astype(jnp.float32)).astype(out.dtype)

        @pl.when(jnp.logical_not(at_end(spot)))
        def _():
            both = near[:, :width].astype(jnp.float32) + far[...].astype(jnp.float32)
            out[rows] = (total + both).astype(out.dtype)


def line_body(tokens, expert_ids, gate_probs, placed, w_gate, w_up, w_down):
    tok_rows, width = tokens.shape
    devices = lax.axis_size("exp")
    here = lax.axis_index("exp")
    last = devices // CORES - 1
    half = tok_rows // 2
    part = half // 2
    spot = here.reshape(1).astype(jnp.int32)
    vmem = pl.BlockSpec(memory_space=pltpu.VMEM)
    smem = pl.BlockSpec(memory_space=pltpu.SMEM)

    def small(kernel, shape, *operands, extra=()):
        return pl.pallas_call(
            kernel,
            in_specs=[smem] + [vmem] * (len(operands) + len(extra)),
            out_specs=vmem,
            out_shape=jax.ShapeDtypeStruct(shape, jnp.bfloat16),
            cost_estimate=pl.CostEstimate(flops=shape[0] * shape[1] * 100, bytes_accessed=0, transcendentals=0),
            compiler_params=pltpu.CompilerParams(vmem_limit_bytes=8 << 20),
        )(spot, *operands, *extra)

    def spread(pairs):
        return [(CORES * a + c, CORES * b + c) for a, b in pairs for c in range(CORES)]

    pair = spread([(0, 1), (1, 0), (last - 1, last), (last, last - 1)])
    twins = [(i, i ^ 1) for i in range(devices)]
    ends = (0, 1, devices - 2, devices - 1)
    middle = spread([(1, 2), (2, 1)]) + [(i, i ^ 1) for i in ends]

    def send(value, perm):
        return lax.ppermute(value, "exp", perm)

    long = width + LANES
    given = [pltpu.with_memory_space_constraint(v, pltpu.HBM) for v in (placed, tokens, expert_ids.T, gate_probs.T)]
    pieces = pl.pallas_call(
        functools.partial(prepare_kernel, devices),
        in_specs=[pl.BlockSpec(memory_space=pltpu.HBM)] * 4,
        out_specs=[vmem] * 5,
        out_shape=[jax.ShapeDtypeStruct((n, long), jnp.bfloat16) for n in (part,) * 4 + (tok_rows,)],
        scratch_shapes=[pltpu.SMEM(placed.shape, placed.dtype)]
        + [pltpu.VMEM(v.shape, v.dtype) for v in given[1:]]
        + [pltpu.SemaphoreType.DMA((4,))],
        compiler_params=pltpu.CompilerParams(vmem_limit_bytes=8 << 20),
    )(*given)
    own_a, own_b, own = pieces[:2], pieces[2:4], pieces[4]

    def load(source, after):
        return pl.pallas_call(
            load_kernel,
            in_specs=[pl.BlockSpec(memory_space=pltpu.HBM), pl.BlockSpec(memory_space=pl.ANY)],
            out_specs=vmem,
            out_shape=pltpu.VMEM(source.shape[1:], source.dtype),
            scratch_shapes=[pltpu.SemaphoreType.DMA],
            cost_estimate=pl.CostEstimate(flops=source.size * 200, bytes_accessed=0, transcendentals=0),
            compiler_params=pltpu.CompilerParams(vmem_limit_bytes=1 << 20),
        )(pltpu.with_memory_space_constraint(source, pltpu.HBM), after)

    held = [load(w, own) for w in (w_gate, w_up, w_down)]

    def run(block, twin=None):
        count = block.shape[0]
        if twin is None:
            twin = send(block, twins)
        call = pl.pallas_call(
            functools.partial(run_kernel, width, devices),
            in_specs=[smem] + [vmem] * 5,
            out_specs=[vmem, vmem],
            out_shape=[
                jax.ShapeDtypeStruct((count, width), jnp.float32),
                jax.ShapeDtypeStruct((count, width), jnp.bfloat16),
            ],
            scratch_shapes=[pltpu.VMEM((2 * count, long), jnp.bfloat16)],
            cost_estimate=pl.CostEstimate(
                flops=count * width * w_gate.shape[2] * 3, bytes_accessed=0, transcendentals=0
            ),
            compiler_params=pltpu.CompilerParams(vmem_limit_bytes=count * (160 << 10)),
        )
        mine, other = call(spot, block, twin, *held)
        return mine, send(other, twins)

    g = [[None, None] for _ in range(8)]
    m = [[None, None] for _ in range(8)]
    near_a = mid_a = far_a = far_b = mid_b = near_b = None

    def start(slot, n):
        first = n * part

        def over(sums, passed):
            return small(functools.partial(over_kernel, first), (part, long), *sums, passed)

        def between(sums, other):
            return small(functools.partial(add_kernel, first), (part, width), *sums, other)

        def ends(outer_sums, inner_sums, other):
            kernel = functools.partial(ends_kernel, first)
            return small(kernel, (part, width), *outer_sums, *inner_sums, other)

        if slot == 0:
            pair_rows, middle_rows = own_a[n], own_a[n]
        elif slot == 1:
            pair_rows = small(pass_kernel, (part, long), own_b[n], m[0][n])
            middle_rows = g[0][n]
        elif slot == 2:
            pair_rows, middle_rows = over(near_a, m[1][n]), g[1][n]
        elif slot == 3:
            pair_rows, middle_rows = over(mid_a, m[2][n]), own_b[n]
        elif slot == 4:
            pair_rows, middle_rows = over(far_a, m[3][n]), between(mid_a, g[3][n])
        elif slot == 5:
            pair_rows, middle_rows = over(far_b, own_b[n]), between(far_a, g[4][n])
        elif slot == 6:
            pair_rows, middle_rows = ends(mid_b, near_a, m[5][n]), between(far_b, g[5][n])
        else:
            pair_rows, middle_rows = ends(near_b, near_b, m[6][n]), between(mid_b, g[6][n])
        g[slot][n] = send(pair_rows, pair)
        m[slot][n] = send(middle_rows, middle)

    def after(slot, n, result):
        g[slot][n], m[slot][n], result = lax.optimization_barrier((g[slot][n], m[slot][n], result))
        return result

    def block(outer_rows, inner_rows):
        return small(join_kernel, (half, long), *outer_rows, *inner_rows, extra=(gates[-1],))

    gates = [jnp.zeros((8, LANES), jnp.int32)]

    def gate():
        call = pl.pallas_call(
            gate_kernel,
            in_specs=[vmem],
            out_specs=vmem,
            out_shape=jax.ShapeDtypeStruct((8, LANES), jnp.int32),
            compiler_params=pltpu.CompilerParams(vmem_limit_bytes=1 << 20),
        )
        gates.append(call(gates[-1]))

    start(0, 0)
    start(0, 1)
    after(0, 0, ())
    start(1, 0)
    gate()
    after(0, 1, ())
    start(1, 1)
    near_a = after(1, 0, run(block(g[0], g[0])))
    start(2, 0)
    gate()
    after(1, 1, ())
    start(2, 1)
    mid_a = after(2, 0, run(block(g[1], m[0])))
    start(3, 0)
    gate()
    after(2, 1, ())
    start(3, 1)
    far_a = after(3, 0, run(block(g[2], m[1])))
    start(4, 0)
    gate()
    after(3, 1, ())
    start(4, 1)
    far_b = after(4, 0, run(block(g[3], m[2])))
    start(5, 0)
    gate()
    after(4, 1, ())
    start(5, 1)
    mid_b = after(5, 0, run(block(g[4], m[3])))
    start(6, 0)
    gate()
    after(5, 1, ())
    start(6, 1)
    near_b = after(6, 0, run(block(g[5], g[1])))
    start(7, 0)
    gate()
    after(6, 1, ())
    start(7, 1)
    mine, back = run(own)
    ends = []
    for n in range(2):
        ends += [g[6][n], g[2][n], m[4][n]]
    for n in range(2):
        ends += [g[7][n], g[7][n], m[7][n]]
    return small(finish_kernel, (tok_rows, width), mine, back, *ends, extra=(gates[-1],))


def body(tokens, *rest):
    if lax.axis_size("exp") == CORES * LINE:
        return line_body(tokens, *rest)
    return sparse_body(tokens, *rest)


def solution(mesh):
    return jax.shard_map(
        body,
        mesh=mesh,
        in_specs=(
            P(("rep", "exp"), None),
            P(("rep", "exp"), None),
            P(("rep", "exp"), None),
            P(),
            P("exp", None, None),
            P("exp", None, None),
            P("exp", None, None),
        ),
        out_specs=P(("rep", "exp"), None),
        check_vma=False,
    )
```

```python
import functools
import jax
import jax.numpy as jnp
from jax import lax
from jax.experimental import pallas as pl
from jax.experimental.pallas import tpu as pltpu
from jax.sharding import PartitionSpec as P


TOK_DEV = 128
CORES = 2
LINE = 4
LANES = 128


def expert_rows(rows, gate_w, up_w, down_w):
    gate = jnp.dot(rows, gate_w, preferred_element_type=jnp.float32)
    up = jnp.dot(rows, up_w, preferred_element_type=jnp.float32)
    hidden = (jax.nn.silu(gate) * up).astype(jnp.bfloat16)
    return jnp.dot(hidden, down_w, preferred_element_type=jnp.float32).astype(jnp.bfloat16)


def run_expert(received, gate_w, up_w, down_w):
    sources, room, width = received.shape
    total_rows = sources * room
    flat = received.reshape(total_rows, width)
    result = expert_rows(flat, gate_w, up_w, down_w)
    return result.reshape(sources, room, width)


def sparse_body(tokens, expert_ids, gate_probs, placed, w_gate, w_up, w_down):
    tok_rows, width = tokens.shape
    picks = expert_ids.shape[1]
    devices = lax.axis_size("exp")
    average = tok_rows * picks // devices
    room = average + max(1, tok_rows * picks // (2 * devices))
    here = lax.axis_index("exp")
    mine = placed[here]
    gate_w, up_w, down_w = (w_gate[0], w_up[0], w_down[0])
    numbers = jnp.arange(devices, dtype=jnp.int32)
    home = jnp.sum(jnp.where(placed[None, :] == numbers[:, None], numbers[None, :], 0), axis=1)
    flat_ids = expert_ids.reshape(-1)
    target_dev = jnp.take(home, flat_ids)
    one_hot = (target_dev[:, None] == numbers[None, :]).astype(jnp.int32)
    rank = jnp.sum((jnp.cumsum(one_hot, axis=0) - 1) * one_hot, axis=1)
    slot_index = target_dev * room + rank
    rows_x = lax.all_gather(tokens, "exp", axis=0, tiled=True)
    rows_ids = lax.all_gather(expert_ids.astype(jnp.bfloat16), "exp", axis=0, tiled=True)
    shards = rows_x.shape[0] // TOK_DEV
    match = rows_ids.astype(jnp.int32).reshape(shards, TOK_DEV * picks) == mine
    order = jnp.cumsum(match.astype(jnp.int32), axis=1) - 1
    spot = jnp.where(match, order, room)
    within = jnp.broadcast_to(
        (jnp.arange(TOK_DEV * picks, dtype=jnp.int32) // picks)[None, :], (shards, TOK_DEV * picks)
    )
    shard_num = jnp.broadcast_to(
        jnp.arange(shards, dtype=jnp.int32)[:, None], (shards, TOK_DEV * picks)
    )
    slot_tok = (
        jnp.full((shards, room), TOK_DEV, jnp.int32).at[shard_num, spot].set(within, mode="drop")
    )
    global_row = jnp.where(
        slot_tok < TOK_DEV,
        jnp.arange(shards, dtype=jnp.int32)[:, None] * TOK_DEV + slot_tok,
        shards * TOK_DEV,
    )
    got = jnp.take(rows_x, global_row.reshape(-1), axis=0, mode="fill", fill_value=0)
    got = got.reshape(shards, room, width)
    counts = jnp.sum(match, axis=1)
    received = got
    produced = run_expert(received, gate_w, up_w, down_w)
    returned = lax.all_to_all(produced, "exp", split_axis=0, concat_axis=0, tiled=True)
    picked = jnp.take(returned.reshape(devices * room, width), slot_index, axis=0)
    picked = picked.reshape(tok_rows, picks, width)
    mixed = jnp.einsum("tk,tkd->td", gate_probs, picked.astype(jnp.float32))
    return mixed.astype(jnp.bfloat16)


def run_kernel(width, devices, spot, block, twin, gate_w, up_w, down_w, own, other, rows):
    half = own.shape[0]
    rows[:half] = block[...]
    rows[half:] = twin[...]
    lane = lax.broadcasted_iota(jnp.int32, (2 * half, LANES), 1)
    mine = (lane == spot[0]) | (lane == spot[0] + devices)
    weights = rows[:, width:].astype(jnp.float32)
    scale = jnp.sum(jnp.where(mine, weights, 0.0), axis=1, keepdims=True)
    x = rows[:, :width]
    gate = jnp.dot(x, gate_w[...], preferred_element_type=jnp.float32)
    up = jnp.dot(x, up_w[...], preferred_element_type=jnp.float32)
    hidden = (gate / (1.0 + jnp.exp(-gate)) * up).astype(jnp.bfloat16)
    result = jnp.dot(hidden, down_w[...], preferred_element_type=jnp.float32) * scale
    own[...] = result[:half]
    other[...] = result[half:].astype(jnp.bfloat16)


def at_end(spot):
    return (spot[0] < CORES) | (spot[0] >= CORES * (LINE - 1))


def load_kernel(count, *refs):
    sources, held, sems = refs[:count], refs[count + 1 : -1], refs[-1]
    copies = [pltpu.make_async_copy(sources[n].at[0], held[n], sems.at[n]) for n in range(count)]
    for copy in copies:
        copy.start()
    for copy in copies:
        copy.wait()


def prepare_kernel(devices, starts, placed_hbm, tokens_hbm, ids_hbm, probs_hbm, after, *refs):
    outs, (placed, ids, probs, sems) = refs[: len(starts)], refs[len(starts) :]
    count, width = ids.shape[1], tokens_hbm.shape[1]
    moves = [(placed_hbm, placed), (ids_hbm, ids), (probs_hbm, probs)]
    for first, out in zip(starts, outs):
        moves.append((tokens_hbm.at[pl.ds(first, out.shape[0])], out.at[:, pl.ds(0, width)]))
    copies = [pltpu.make_async_copy(src, dst, sems.at[n]) for n, (src, dst) in enumerate(moves)]
    for copy in copies:
        copy.start()
    for copy in copies[:3]:
        copy.wait()
    slot = lax.broadcasted_iota(jnp.int32, (LANES, count), 0)
    weight = jnp.zeros((LANES, count), jnp.float32)
    for s in range(devices):
        total = jnp.zeros((1, count), jnp.float32)
        for k in range(ids.shape[0]):
            total += jnp.where(ids[k : k + 1, :] == placed[s], probs[k : k + 1, :], 0.0)
        high = total.astype(jnp.bfloat16).astype(jnp.float32)
        weight = jnp.where(slot == s, high, jnp.where(slot == s + devices, total - high, weight))
    packed = weight.T.astype(jnp.bfloat16)
    for first, out in zip(starts, outs):
        out[:, width:] = packed[first : first + out.shape[0], :]
    for copy in copies[3:]:
        copy.wait()


def gate_kernel(before, out):
    out[...] = before[...]


def join_kernel(spot, outer_x, outer_y, inner_x, inner_y, gate, out):
    part = outer_x.shape[0]

    @pl.when(at_end(spot))
    def _():
        out[:part] = outer_x[...]
        out[part:] = outer_y[...]

    @pl.when(jnp.logical_not(at_end(spot)))
    def _():
        out[:part] = inner_x[...]
        out[part:] = inner_y[...]


def over_kernel(start, spot, own, back, passed, out):
    part, width = out.shape[0], own.shape[1]

    @pl.when(at_end(spot))
    def _():
        total = own[start : start + part] + back[start : start + part].astype(jnp.float32)
        out[:, :width] = total.astype(out.dtype)
        out[:, width:] = jnp.zeros((part, out.shape[1] - width), out.dtype)

    @pl.when(jnp.logical_not(at_end(spot)))
    def _():
        out[...] = passed[...]


def pass_kernel(spot, mine, passed, out):
    @pl.when(at_end(spot))
    def _():
        out[...] = mine[...]

    @pl.when(jnp.logical_not(at_end(spot)))
    def _():
        out[...] = passed[...]


def add_kernel(start, spot, own, back, other, out):
    part, width = out.shape
    total = own[start : start + part] + back[start : start + part].astype(jnp.float32)
    out[...] = (total + other[:, :width].astype(jnp.float32)).astype(out.dtype)


def ends_kernel(start, spot, outer_own, outer_back, inner_own, inner_back, other, out):
    part = out.shape[0]

    @pl.when(at_end(spot))
    def _():
        total = outer_own[start : start + part] + outer_back[start : start + part].astype(jnp.float32)
        out[...] = total.astype(out.dtype)

    @pl.when(jnp.logical_not(at_end(spot)))
    def _():
        total = inner_own[start : start + part] + inner_back[start : start + part].astype(jnp.float32)
        out[...] = (total + other[...].astype(jnp.float32)).astype(out.dtype)


def finish_kernel(first, start, parts, spot, own, back, *refs):
    out, total, sem = refs[-3:]
    part, width = refs[0].shape
    for n in range(parts):
        sums, near, far = refs[3 * n : 3 * n + 3]
        rows = slice(n * part, (n + 1) * part)
        mine = slice(start + n * part, start + (n + 1) * part)
        share = own[mine] + back[mine].astype(jnp.float32)

        @pl.when(at_end(spot))
        def _():
            total[rows] = (share + sums[...].astype(jnp.float32)).astype(out.dtype)

        @pl.when(jnp.logical_not(at_end(spot)))
        def _():
            both = near[:, :width].astype(jnp.float32) + far[...].astype(jnp.float32)
            total[rows] = (share + both).astype(out.dtype)

    copy = pltpu.make_async_copy(total, out.at[pl.ds(first, parts * part)], sem)
    copy.start()
    copy.wait()


def line_body(tokens, expert_ids, gate_probs, placed, w_gate, w_up, w_down):
    tok_rows, width = tokens.shape
    devices = lax.axis_size("exp")
    here = lax.axis_index("exp")
    chip = here // CORES
    last = devices // CORES - 1
    outer = (chip == 0) | (chip == last)
    half = tok_rows // 2
    part = half // 2
    spot = here.reshape(1).astype(jnp.int32)
    vmem = pl.BlockSpec(memory_space=pltpu.VMEM)
    smem = pl.BlockSpec(memory_space=pltpu.SMEM)

    def small(kernel, shape, *operands, extra=()):
        return pl.pallas_call(
            kernel,
            in_specs=[smem] + [vmem] * (len(operands) + len(extra)),
            out_specs=vmem,
            out_shape=jax.ShapeDtypeStruct(shape, jnp.bfloat16),
            cost_estimate=pl.CostEstimate(flops=shape[0] * shape[1] * 100, bytes_accessed=0, transcendentals=0),
            compiler_params=pltpu.CompilerParams(vmem_limit_bytes=8 << 20),
        )(spot, *operands, *extra)

    def spread(pairs):
        return [(CORES * a + c, CORES * b + c) for a, b in pairs for c in range(CORES)]

    pair = spread([(0, 1), (1, 0), (last - 1, last), (last, last - 1)])
    twins = [(i, i ^ 1) for i in range(devices)]
    ends = (0, 1, devices - 2, devices - 1)
    middle = spread([(1, 2), (2, 1)]) + [(i, i ^ 1) for i in ends]

    def send(value, perm):
        return lax.ppermute(value, "exp", perm)

    long = width + LANES
    given = [pltpu.with_memory_space_constraint(v, pltpu.HBM) for v in (placed, tokens, expert_ids.T, gate_probs.T)]

    def prepare(pieces, after):
        starts, sizes = zip(*pieces)
        return pl.pallas_call(
            functools.partial(prepare_kernel, devices, starts),
            in_specs=[pl.BlockSpec(memory_space=pltpu.HBM)] * 4 + [pl.BlockSpec(memory_space=pl.ANY)],
            out_specs=[vmem] * len(pieces),
            out_shape=[jax.ShapeDtypeStruct((size, long), jnp.bfloat16) for size in sizes],
            scratch_shapes=[pltpu.SMEM(placed.shape, placed.dtype)]
            + [pltpu.VMEM(v.shape, v.dtype) for v in given[2:]]
            + [pltpu.SemaphoreType.DMA((3 + len(pieces),))],
            compiler_params=pltpu.CompilerParams(vmem_limit_bytes=4 << 20),
        )(*given, after)

    own_a = prepare([(0, part), (part, part)], given[0])
    own_b = prepare([(half, part), (half + part, part), (0, half), (half, half)], own_a[0])
    own_b, own_whole = own_b[:2], own_b[2:]

    hbm = pl.BlockSpec(memory_space=pltpu.HBM)

    def load(sources, after):
        count = len(sources)
        return pl.pallas_call(
            functools.partial(load_kernel, count),
            in_specs=[hbm] * count + [pl.BlockSpec(memory_space=pl.ANY)],
            out_specs=[vmem] * count,
            out_shape=[pltpu.VMEM(w.shape[1:], w.dtype) for w in sources],
            scratch_shapes=[pltpu.SemaphoreType.DMA((count,))],
            cost_estimate=pl.CostEstimate(
                flops=count * sources[0].size * 200, bytes_accessed=0, transcendentals=0
            ),
            compiler_params=pltpu.CompilerParams(vmem_limit_bytes=1 << 20),
        )(*[pltpu.with_memory_space_constraint(w, pltpu.HBM) for w in sources], after)

    held = load((w_gate, w_up), own_a[0])
    held += load((w_down,), own_a[0])

    def run(block):
        count = block.shape[0]
        twin = send(block, twins)
        call = pl.pallas_call(
            functools.partial(run_kernel, width, devices),
            in_specs=[smem] + [vmem] * 5,
            out_specs=[vmem, vmem],
            out_shape=[
                jax.ShapeDtypeStruct((count, width), jnp.float32),
                jax.ShapeDtypeStruct((count, width), jnp.bfloat16),
            ],
            scratch_shapes=[pltpu.VMEM((2 * count, long), jnp.bfloat16)],
            cost_estimate=pl.CostEstimate(
                flops=count * width * w_gate.shape[2] * 3, bytes_accessed=0, transcendentals=0
            ),
            compiler_params=pltpu.CompilerParams(vmem_limit_bytes=count * (160 << 10)),
        )
        mine, other = call(spot, block, twin, *held)
        return mine, send(other, twins)

    g = [[None, None] for _ in range(8)]
    m = [[None, None] for _ in range(8)]
    near_a = mid_a = far_a = far_b = mid_b = near_b = None

    def start(slot, n):
        first = n * part

        def over(sums, passed):
            return small(functools.partial(over_kernel, first), (part, long), *sums, passed)

        def between(sums, other):
            return small(functools.partial(add_kernel, first), (part, width), *sums, other)

        def ends(outer_sums, inner_sums, other):
            kernel = functools.partial(ends_kernel, first)
            return small(kernel, (part, width), *outer_sums, *inner_sums, other)

        if slot == 0:
            pair_rows, middle_rows = own_a[n], own_a[n]
        elif slot == 1:
            pair_rows = small(pass_kernel, (part, long), own_b[n], m[0][n])
            middle_rows = g[0][n]
        elif slot == 2:
            pair_rows, middle_rows = over(near_a, m[1][n]), g[1][n]
        elif slot == 3:
            pair_rows, middle_rows = over(mid_a, m[2][n]), own_b[n]
        elif slot == 4:
            pair_rows, middle_rows = over(far_a, m[3][n]), between(mid_a, g[3][n])
        elif slot == 5:
            pair_rows, middle_rows = over(far_b, own_b[n]), between(far_a, g[4][n])
        elif slot == 6:
            pair_rows, middle_rows = ends(mid_b, near_a, m[5][n]), between(far_b, g[5][n])
        else:
            pair_rows, middle_rows = ends(near_b, near_b, m[6][n]), between(mid_b, g[6][n])
        g[slot][n] = send(pair_rows, pair)
        m[slot][n] = send(middle_rows, middle)

    def after(slot, n, result):
        g[slot][n], m[slot][n], mine = lax.optimization_barrier((g[slot][n], m[slot][n], result[:1]))
        return mine + result[1:]

    def block(outer_rows, inner_rows):
        return small(join_kernel, (half, long), *outer_rows, *inner_rows, extra=(gates[-1],))

    gates = [jnp.zeros((8, LANES), jnp.int32)]

    def gate():
        call = pl.pallas_call(
            gate_kernel,
            in_specs=[vmem],
            out_specs=vmem,
            out_shape=jax.ShapeDtypeStruct((8, LANES), jnp.int32),
            compiler_params=pltpu.CompilerParams(vmem_limit_bytes=1 << 20),
        )
        gates.append(call(gates[-1]))

    start(0, 0)
    start(0, 1)
    here_a = run(own_whole[0])
    after(0, 0, ())
    start(1, 0)
    gate()
    start(1, 1)
    near_a = after(1, 0, run(block(g[0], g[0])))
    start(2, 0)
    gate()
    start(2, 1)
    mid_a = after(2, 0, run(block(g[1], m[0])))
    start(3, 0)
    gate()
    start(3, 1)
    far_a = after(3, 0, run(block(g[2], m[1])))
    start(4, 0)
    gate()
    start(4, 1)
    far_b = after(4, 0, run(block(g[3], m[2])))
    start(5, 0)
    gate()
    start(5, 1)
    mid_b = after(5, 0, run(block(g[4], m[3])))
    start(6, 0)
    gate()
    start(6, 1)
    near_b = after(6, 0, run(block(g[5], g[1])))
    start(7, 0)
    gate()
    start(7, 1)
    here_b = run(own_whole[1])

    def finish(first, sums, ends, *extra):
        operands = (*sums, *(v for triple in ends for v in triple))
        parts = len(ends)
        return pl.pallas_call(
            functools.partial(finish_kernel, first, first % half, parts),
            in_specs=[smem] + [vmem] * len(operands) + [pl.BlockSpec(memory_space=pl.ANY)] * len(extra),
            out_specs=hbm,
            out_shape=jax.ShapeDtypeStruct((tok_rows, width), jnp.bfloat16),
            scratch_shapes=[pltpu.VMEM((parts * part, width), jnp.bfloat16), pltpu.SemaphoreType.DMA],
            input_output_aliases={len(operands) + 1: 0} if first else {},
            compiler_params=pltpu.CompilerParams(vmem_limit_bytes=8 << 20),
        )(spot, *operands, *extra)

    rows = finish(0, here_a, [(g[6][n], g[2][n], m[4][n]) for n in range(2)], gates[-1])
    rows = finish(half, here_b, [(g[7][0], g[7][0], m[7][0])], rows)
    return finish(half + part, here_b, [(g[7][1], g[7][1], m[7][1])], rows)


def body(tokens, *rest):
    if lax.axis_size("exp") == CORES * LINE:
        return line_body(tokens, *rest)
    return sparse_body(tokens, *rest)


def solution(mesh):
    return jax.shard_map(
        body,
        mesh=mesh,
        in_specs=(
            P(("rep", "exp"), None),
            P(("rep", "exp"), None),
            P(("rep", "exp"), None),
            P(),
            P("exp", None, None),
            P("exp", None, None),
            P("exp", None, None),
        ),
        out_specs=P(("rep", "exp"), None),
        check_vma=False,
    )
```

```python
import functools
import jax
import jax.numpy as jnp
from jax import lax
from jax.experimental import pallas as pl
from jax.experimental.pallas import tpu as pltpu
from jax.sharding import PartitionSpec as P


TOK_DEV = 128
CORES = 2
LINE = 4
LANES = 128


def expert_rows(rows, gate_w, up_w, down_w):
    gate = jnp.dot(rows, gate_w, preferred_element_type=jnp.float32)
    up = jnp.dot(rows, up_w, preferred_element_type=jnp.float32)
    hidden = (jax.nn.silu(gate) * up).astype(jnp.bfloat16)
    return jnp.dot(hidden, down_w, preferred_element_type=jnp.float32).astype(jnp.bfloat16)


def run_expert(received, gate_w, up_w, down_w):
    sources, room, width = received.shape
    total_rows = sources * room
    flat = received.reshape(total_rows, width)
    result = expert_rows(flat, gate_w, up_w, down_w)
    return result.reshape(sources, room, width)


def sparse_body(tokens, expert_ids, gate_probs, placed, w_gate, w_up, w_down):
    tok_rows, width = tokens.shape
    picks = expert_ids.shape[1]
    devices = lax.axis_size("exp")
    average = tok_rows * picks // devices
    room = average + max(1, tok_rows * picks // (2 * devices))
    here = lax.axis_index("exp")
    mine = placed[here]
    gate_w, up_w, down_w = (w_gate[0], w_up[0], w_down[0])
    numbers = jnp.arange(devices, dtype=jnp.int32)
    home = jnp.sum(jnp.where(placed[None, :] == numbers[:, None], numbers[None, :], 0), axis=1)
    flat_ids = expert_ids.reshape(-1)
    target_dev = jnp.take(home, flat_ids)
    one_hot = (target_dev[:, None] == numbers[None, :]).astype(jnp.int32)
    rank = jnp.sum((jnp.cumsum(one_hot, axis=0) - 1) * one_hot, axis=1)
    slot_index = target_dev * room + rank
    rows_x = lax.all_gather(tokens, "exp", axis=0, tiled=True)
    rows_ids = lax.all_gather(expert_ids.astype(jnp.bfloat16), "exp", axis=0, tiled=True)
    shards = rows_x.shape[0] // TOK_DEV
    match = rows_ids.astype(jnp.int32).reshape(shards, TOK_DEV * picks) == mine
    order = jnp.cumsum(match.astype(jnp.int32), axis=1) - 1
    spot = jnp.where(match, order, room)
    within = jnp.broadcast_to(
        (jnp.arange(TOK_DEV * picks, dtype=jnp.int32) // picks)[None, :], (shards, TOK_DEV * picks)
    )
    shard_num = jnp.broadcast_to(
        jnp.arange(shards, dtype=jnp.int32)[:, None], (shards, TOK_DEV * picks)
    )
    slot_tok = (
        jnp.full((shards, room), TOK_DEV, jnp.int32).at[shard_num, spot].set(within, mode="drop")
    )
    global_row = jnp.where(
        slot_tok < TOK_DEV,
        jnp.arange(shards, dtype=jnp.int32)[:, None] * TOK_DEV + slot_tok,
        shards * TOK_DEV,
    )
    got = jnp.take(rows_x, global_row.reshape(-1), axis=0, mode="fill", fill_value=0)
    got = got.reshape(shards, room, width)
    counts = jnp.sum(match, axis=1)
    received = got
    produced = run_expert(received, gate_w, up_w, down_w)
    returned = lax.all_to_all(produced, "exp", split_axis=0, concat_axis=0, tiled=True)
    picked = jnp.take(returned.reshape(devices * room, width), slot_index, axis=0)
    picked = picked.reshape(tok_rows, picks, width)
    mixed = jnp.einsum("tk,tkd->td", gate_probs, picked.astype(jnp.float32))
    return mixed.astype(jnp.bfloat16)


def run_kernel(width, devices, spot, block, twin, gate_w, up_w, down_w, own, other_x, other_y, rows):
    half = own.shape[0]
    rows[:half] = block[...]
    rows[half:] = twin[...]
    lane = lax.broadcasted_iota(jnp.int32, (2 * half, LANES), 1)
    row = lax.broadcasted_iota(jnp.int32, (2 * half, LANES), 0)
    part = half // 2
    lower = ((row >= part) & (row < half)) | (row >= half + part)
    lane = jnp.where(lower, lane - 2 * devices, lane)
    mine = (lane == spot[0]) | (lane == spot[0] + devices)
    weights = rows[:, width:].astype(jnp.float32)
    scale = jnp.sum(jnp.where(mine, weights, 0.0), axis=1, keepdims=True)
    x = rows[:, :width]
    gate = jnp.dot(x, gate_w[...], preferred_element_type=jnp.float32)
    up = jnp.dot(x, up_w[...], preferred_element_type=jnp.float32)
    hidden = (gate / (1.0 + jnp.exp(-gate)) * up).astype(jnp.bfloat16)
    result = jnp.dot(hidden, down_w[...], preferred_element_type=jnp.float32) * scale
    own[...] = result[:half]
    other_x[...] = result[half : half + part].astype(jnp.bfloat16)
    other_y[...] = result[half + part :].astype(jnp.bfloat16)


def at_end(spot):
    return (spot[0] < CORES) | (spot[0] >= CORES * (LINE - 1))


def load_kernel(count, *refs):
    sources, held, sems = refs[:count], refs[count + 1 : -1], refs[-1]
    copies = [pltpu.make_async_copy(sources[n].at[0], held[n], sems.at[n]) for n in range(count)]
    for copy in copies:
        copy.start()
    for copy in copies:
        copy.wait()


def prepare_kernel(devices, part, starts, placed_hbm, tokens_hbm, ids_hbm, probs_hbm, after, *refs):
    outs, (placed, ids, probs, sems) = refs[: len(starts)], refs[len(starts) :]
    count, width = ids.shape[1], tokens_hbm.shape[1]
    moves = [(placed_hbm, placed), (ids_hbm, ids), (probs_hbm, probs)]
    for first, out in zip(starts, outs):
        moves.append((tokens_hbm.at[pl.ds(first, out.shape[0])], out.at[:, pl.ds(0, width)]))
    copies = [pltpu.make_async_copy(src, dst, sems.at[n]) for n, (src, dst) in enumerate(moves)]
    for copy in copies:
        copy.start()
    for copy in copies[:3]:
        copy.wait()
    slot = lax.broadcasted_iota(jnp.int32, (LANES, count), 0)
    weight = jnp.zeros((LANES, count), jnp.float32)
    for s in range(devices):
        total = jnp.zeros((1, count), jnp.float32)
        for k in range(ids.shape[0]):
            total += jnp.where(ids[k : k + 1, :] == placed[s], probs[k : k + 1, :], 0.0)
        high = total.astype(jnp.bfloat16).astype(jnp.float32)
        for base in (s, s + 2 * devices):
            weight = jnp.where(slot == base, high, jnp.where(slot == base + devices, total - high, weight))
    packed = weight.T.astype(jnp.bfloat16)
    lane = lax.broadcasted_iota(jnp.int32, (part, LANES), 1)
    for first, out in zip(starts, outs):
        if out.shape[1] > width:
            upper = packed[first : first + part, :]
            lower = packed[first + part : first + 2 * part, :]
            both = jnp.where(lane < 2 * devices, upper.astype(jnp.float32), lower.astype(jnp.float32))
            for row in range(0, out.shape[0], part):
                out[row : row + part, width:] = both.astype(jnp.bfloat16)
    for copy in copies[3:]:
        copy.wait()


def gate_kernel(before, out):
    out[...] = before[...]


def join_kernel(spot, outer_x, outer_y, inner_x, inner_y, gate, out):
    part, width = outer_y.shape

    def put(upper, lower):
        out[:part] = upper[...]
        out[part:, :width] = lower[...]
        out[part:, width:] = upper[:, width:]

    @pl.when(at_end(spot))
    def _():
        put(outer_x, outer_y)

    @pl.when(jnp.logical_not(at_end(spot)))
    def _():
        put(inner_x, inner_y)


def over_kernel(start, spot, own, back, passed, out):
    part, width = out.shape[0], own.shape[1]

    @pl.when(at_end(spot))
    def _():
        total = own[start : start + part] + back[...].astype(jnp.float32)
        out[:, :width] = total.astype(out.dtype)
        if out.shape[1] > width:
            out[:, width:] = jnp.zeros((part, out.shape[1] - width), out.dtype)

    @pl.when(jnp.logical_not(at_end(spot)))
    def _():
        out[...] = passed[...]


def pass_kernel(spot, mine, passed, out):
    @pl.when(at_end(spot))
    def _():
        out[...] = mine[...]

    @pl.when(jnp.logical_not(at_end(spot)))
    def _():
        out[...] = passed[...]


def add_kernel(start, spot, own, back, other, out):
    part, width = out.shape
    total = own[start : start + part] + back[...].astype(jnp.float32)
    out[...] = (total + other[:, :width].astype(jnp.float32)).astype(out.dtype)


def ends_kernel(start, spot, outer_own, outer_back, inner_own, inner_back, other, out):
    part = out.shape[0]

    @pl.when(at_end(spot))
    def _():
        total = outer_own[start : start + part] + outer_back[...].astype(jnp.float32)
        out[...] = total.astype(out.dtype)

    @pl.when(jnp.logical_not(at_end(spot)))
    def _():
        total = inner_own[start : start + part] + inner_back[...].astype(jnp.float32)
        out[...] = (total + other[...].astype(jnp.float32)).astype(out.dtype)


def finish_kernel(first, start, parts, spot, own, *refs):
    backs, refs, (out, total, sem) = refs[:parts], refs[parts:-3], refs[-3:]
    part, width = refs[0].shape
    for n in range(parts):
        sums, near, far = refs[3 * n : 3 * n + 3]
        rows = slice(n * part, (n + 1) * part)
        mine = slice(start + n * part, start + (n + 1) * part)
        share = own[mine] + backs[n][...].astype(jnp.float32)

        @pl.when(at_end(spot))
        def _():
            total[rows] = (share + sums[...].astype(jnp.float32)).astype(out.dtype)

        @pl.when(jnp.logical_not(at_end(spot)))
        def _():
            both = near[:, :width].astype(jnp.float32) + far[...].astype(jnp.float32)
            total[rows] = (share + both).astype(out.dtype)

    copy = pltpu.make_async_copy(total, out.at[pl.ds(first, parts * part)], sem)
    copy.start()
    copy.wait()


def line_body(tokens, expert_ids, gate_probs, placed, w_gate, w_up, w_down):
    tok_rows, width = tokens.shape
    devices = lax.axis_size("exp")
    here = lax.axis_index("exp")
    last = devices // CORES - 1
    half = tok_rows // 2
    part = half // 2
    spot = here.reshape(1).astype(jnp.int32)
    vmem = pl.BlockSpec(memory_space=pltpu.VMEM)
    smem = pl.BlockSpec(memory_space=pltpu.SMEM)

    def small(kernel, shape, *operands, extra=()):
        return pl.pallas_call(
            kernel,
            in_specs=[smem] + [vmem] * (len(operands) + len(extra)),
            out_specs=vmem,
            out_shape=jax.ShapeDtypeStruct(shape, jnp.bfloat16),
            cost_estimate=pl.CostEstimate(flops=shape[0] * shape[1] * 100, bytes_accessed=0, transcendentals=0),
            compiler_params=pltpu.CompilerParams(vmem_limit_bytes=8 << 20),
        )(spot, *operands, *extra)

    def spread(pairs):
        return [(CORES * a + c, CORES * b + c) for a, b in pairs for c in range(CORES)]

    pair = spread([(0, 1), (1, 0), (last - 1, last), (last, last - 1)])
    twins = [(i, i ^ 1) for i in range(devices)]
    ends = (0, 1, devices - 2, devices - 1)
    middle = spread([(1, 2), (2, 1)]) + [(i, i ^ 1) for i in ends]

    def send(value, perm):
        return lax.ppermute(value, "exp", perm)

    long = width + LANES
    given = [pltpu.with_memory_space_constraint(v, pltpu.HBM) for v in (placed, tokens, expert_ids.T, gate_probs.T)]

    def prepare(pieces, after):
        starts = [first for first, _, _ in pieces]
        return pl.pallas_call(
            functools.partial(prepare_kernel, devices, part, starts),
            in_specs=[pl.BlockSpec(memory_space=pltpu.HBM)] * 4 + [pl.BlockSpec(memory_space=pl.ANY)],
            out_specs=[vmem] * len(pieces),
            out_shape=[jax.ShapeDtypeStruct(shape, jnp.bfloat16) for _, *shape in pieces],
            scratch_shapes=[pltpu.SMEM(placed.shape, placed.dtype)]
            + [pltpu.VMEM(v.shape, v.dtype) for v in given[2:]]
            + [pltpu.SemaphoreType.DMA((3 + len(pieces),))],
            compiler_params=pltpu.CompilerParams(vmem_limit_bytes=4 << 20),
        )(*given, after)

    own_a = prepare([(0, part, long), (part, part, width)], given[0])
    others = [(half, part, long), (half + part, part, width), (0, half, long), (half, half, long)]
    own_b = prepare(others, own_a[0])
    own_b, own_whole = own_b[:2], own_b[2:]

    hbm = pl.BlockSpec(memory_space=pltpu.HBM)

    def load(sources, after):
        count = len(sources)
        return pl.pallas_call(
            functools.partial(load_kernel, count),
            in_specs=[hbm] * count + [pl.BlockSpec(memory_space=pl.ANY)],
            out_specs=[vmem] * count,
            out_shape=[pltpu.VMEM(w.shape[1:], w.dtype) for w in sources],
            scratch_shapes=[pltpu.SemaphoreType.DMA((count,))],
            cost_estimate=pl.CostEstimate(
                flops=count * sources[0].size * 200, bytes_accessed=0, transcendentals=0
            ),
            compiler_params=pltpu.CompilerParams(vmem_limit_bytes=1 << 20),
        )(*[pltpu.with_memory_space_constraint(w, pltpu.HBM) for w in sources], after)

    held = load((w_gate, w_up), own_a[0])
    held += load((w_down,), own_a[0])

    def run(block):
        count = block.shape[0]
        twin = send(block, twins)
        call = pl.pallas_call(
            functools.partial(run_kernel, width, devices),
            in_specs=[smem] + [vmem] * 5,
            out_specs=[vmem] * 3,
            out_shape=[jax.ShapeDtypeStruct((count, width), jnp.float32)]
            + [jax.ShapeDtypeStruct((part, width), jnp.bfloat16)] * 2,
            scratch_shapes=[pltpu.VMEM((2 * count, long), jnp.bfloat16)],
            cost_estimate=pl.CostEstimate(
                flops=count * width * w_gate.shape[2] * 3, bytes_accessed=0, transcendentals=0
            ),
            compiler_params=pltpu.CompilerParams(vmem_limit_bytes=count * (160 << 10)),
        )
        mine, other_x, other_y = call(spot, block, twin, *held)
        return mine, send(other_x, twins), send(other_y, twins)

    g = [[None, None] for _ in range(8)]
    m = [[None, None] for _ in range(8)]
    near_a = mid_a = far_a = far_b = mid_b = near_b = None

    def start(slot, n):
        first = n * part

        def over(sums, passed):
            return small(functools.partial(over_kernel, first), passed.shape, sums[0], sums[1 + n], passed)

        def between(sums, other):
            return small(functools.partial(add_kernel, first), (part, width), sums[0], sums[1 + n], other)

        def ends(outer_sums, inner_sums, other):
            kernel = functools.partial(ends_kernel, first)
            sums = (outer_sums[0], outer_sums[1 + n], inner_sums[0], inner_sums[1 + n])
            return small(kernel, (part, width), *sums, other)

        if slot == 0:
            pair_rows, middle_rows = own_a[n], own_a[n]
        elif slot == 1:
            pair_rows = small(pass_kernel, own_b[n].shape, own_b[n], m[0][n])
            middle_rows = g[0][n]
        elif slot == 2:
            pair_rows, middle_rows = over(near_a, m[1][n]), g[1][n]
        elif slot == 3:
            pair_rows, middle_rows = over(mid_a, m[2][n]), own_b[n]
        elif slot == 4:
            pair_rows, middle_rows = over(far_a, m[3][n]), between(mid_a, g[3][n])
        elif slot == 5:
            pair_rows, middle_rows = over(far_b, own_b[n]), between(far_a, g[4][n])
        elif slot == 6:
            pair_rows, middle_rows = ends(mid_b, near_a, m[5][n]), between(far_b, g[5][n])
        else:
            pair_rows, middle_rows = ends(near_b, near_b, m[6][n]), between(mid_b, g[6][n])
        g[slot][n] = send(pair_rows, pair)
        m[slot][n] = send(middle_rows, middle)

    def after(slot, n, result):
        g[slot][n], m[slot][n], mine = lax.optimization_barrier((g[slot][n], m[slot][n], result[:1]))
        return mine + result[1:]

    def block(outer_rows, inner_rows):
        return small(join_kernel, (half, long), *outer_rows, *inner_rows, extra=(gates[-1],))

    gates = [jnp.zeros((8, LANES), jnp.int32)]

    def gate():
        call = pl.pallas_call(
            gate_kernel,
            in_specs=[vmem],
            out_specs=vmem,
            out_shape=jax.ShapeDtypeStruct((8, LANES), jnp.int32),
            compiler_params=pltpu.CompilerParams(vmem_limit_bytes=1 << 20),
        )
        gates.append(call(gates[-1]))

    start(0, 0)
    start(0, 1)
    here_a = run(own_whole[0])
    after(0, 0, ())
    start(1, 0)
    gate()
    start(1, 1)
    near_a = after(1, 0, run(block(g[0], g[0])))
    start(2, 0)
    gate()
    start(2, 1)
    mid_a = after(2, 0, run(block(g[1], m[0])))
    start(3, 0)
    gate()
    start(3, 1)
    far_a = after(3, 0, run(block(g[2], m[1])))
    start(4, 0)
    gate()
    start(4, 1)
    far_b = after(4, 0, run(block(g[3], m[2])))
    start(5, 0)
    gate()
    start(5, 1)
    mid_b = after(5, 0, run(block(g[4], m[3])))
    start(6, 0)
    gate()
    start(6, 1)
    near_b = after(6, 0, run(block(g[5], g[1])))
    start(7, 0)
    gate()
    start(7, 1)
    here_b = run(own_whole[1])

    def finish(first, sums, ends, *extra):
        operands = (*sums, *(v for triple in ends for v in triple))
        parts = len(ends)
        return pl.pallas_call(
            functools.partial(finish_kernel, first, first % half, parts),
            in_specs=[smem] + [vmem] * len(operands) + [pl.BlockSpec(memory_space=pl.ANY)] * len(extra),
            out_specs=hbm,
            out_shape=jax.ShapeDtypeStruct((tok_rows, width), jnp.bfloat16),
            scratch_shapes=[pltpu.VMEM((parts * part, width), jnp.bfloat16), pltpu.SemaphoreType.DMA],
            input_output_aliases={len(operands) + 1: 0} if first else {},
            compiler_params=pltpu.CompilerParams(vmem_limit_bytes=8 << 20),
        )(spot, *operands, *extra)

    rows = finish(0, here_a, [(g[6][n], g[2][n], m[4][n]) for n in range(2)], gates[-1])
    rows = finish(half, here_b[:2], [(g[7][0], g[7][0], m[7][0])], rows)
    return finish(half + part, here_b[::2], [(g[7][1], g[7][1], m[7][1])], rows)


def body(tokens, *rest):
    if lax.axis_size("exp") == CORES * LINE:
        return line_body(tokens, *rest)
    return sparse_body(tokens, *rest)


def solution(mesh):
    return jax.shard_map(
        body,
        mesh=mesh,
        in_specs=(
            P(("rep", "exp"), None),
            P(("rep", "exp"), None),
            P(("rep", "exp"), None),
            P(),
            P("exp", None, None),
            P("exp", None, None),
            P("exp", None, None),
        ),
        out_specs=P(("rep", "exp"), None),
        check_vma=False,
    )
```

```python
import functools
import jax
import jax.numpy as jnp
from jax import lax
from jax.experimental import pallas as pl
from jax.experimental.pallas import tpu as pltpu
from jax.sharding import PartitionSpec as P


TOK_DEV = 128
CORES = 2
LINE = 4
LANES = 128


def expert_rows(rows, gate_w, up_w, down_w):
    gate = jnp.dot(rows, gate_w, preferred_element_type=jnp.float32)
    up = jnp.dot(rows, up_w, preferred_element_type=jnp.float32)
    hidden = (jax.nn.silu(gate) * up).astype(jnp.bfloat16)
    return jnp.dot(hidden, down_w, preferred_element_type=jnp.float32).astype(jnp.bfloat16)


def run_expert(received, gate_w, up_w, down_w):
    sources, room, width = received.shape
    total_rows = sources * room
    flat = received.reshape(total_rows, width)
    result = expert_rows(flat, gate_w, up_w, down_w)
    return result.reshape(sources, room, width)


def sparse_body(tokens, expert_ids, gate_probs, placed, w_gate, w_up, w_down):
    tok_rows, width = tokens.shape
    picks = expert_ids.shape[1]
    devices = lax.axis_size("exp")
    average = tok_rows * picks // devices
    room = average + max(1, tok_rows * picks // (2 * devices))
    here = lax.axis_index("exp")
    mine = placed[here]
    gate_w, up_w, down_w = (w_gate[0], w_up[0], w_down[0])
    numbers = jnp.arange(devices, dtype=jnp.int32)
    home = jnp.sum(jnp.where(placed[None, :] == numbers[:, None], numbers[None, :], 0), axis=1)
    flat_ids = expert_ids.reshape(-1)
    target_dev = jnp.take(home, flat_ids)
    one_hot = (target_dev[:, None] == numbers[None, :]).astype(jnp.int32)
    rank = jnp.sum((jnp.cumsum(one_hot, axis=0) - 1) * one_hot, axis=1)
    slot_index = target_dev * room + rank
    rows_x = lax.all_gather(tokens, "exp", axis=0, tiled=True)
    rows_ids = lax.all_gather(expert_ids.astype(jnp.bfloat16), "exp", axis=0, tiled=True)
    shards = rows_x.shape[0] // TOK_DEV
    match = rows_ids.astype(jnp.int32).reshape(shards, TOK_DEV * picks) == mine
    order = jnp.cumsum(match.astype(jnp.int32), axis=1) - 1
    spot = jnp.where(match, order, room)
    within = jnp.broadcast_to(
        (jnp.arange(TOK_DEV * picks, dtype=jnp.int32) // picks)[None, :], (shards, TOK_DEV * picks)
    )
    shard_num = jnp.broadcast_to(
        jnp.arange(shards, dtype=jnp.int32)[:, None], (shards, TOK_DEV * picks)
    )
    slot_tok = (
        jnp.full((shards, room), TOK_DEV, jnp.int32).at[shard_num, spot].set(within, mode="drop")
    )
    global_row = jnp.where(
        slot_tok < TOK_DEV,
        jnp.arange(shards, dtype=jnp.int32)[:, None] * TOK_DEV + slot_tok,
        shards * TOK_DEV,
    )
    got = jnp.take(rows_x, global_row.reshape(-1), axis=0, mode="fill", fill_value=0)
    got = got.reshape(shards, room, width)
    counts = jnp.sum(match, axis=1)
    received = got
    produced = run_expert(received, gate_w, up_w, down_w)
    returned = lax.all_to_all(produced, "exp", split_axis=0, concat_axis=0, tiled=True)
    picked = jnp.take(returned.reshape(devices * room, width), slot_index, axis=0)
    picked = picked.reshape(tok_rows, picks, width)
    mixed = jnp.einsum("tk,tkd->td", gate_probs, picked.astype(jnp.float32))
    return mixed.astype(jnp.bfloat16)


def run_kernel(width, devices, spot, block, twin, gate_w, up_w, down_w, own, other_x, other_y, rows):
    half = own.shape[0]
    rows[:half] = block[...]
    rows[half:] = twin[...]
    lane = lax.broadcasted_iota(jnp.int32, (2 * half, LANES), 1)
    row = lax.broadcasted_iota(jnp.int32, (2 * half, LANES), 0)
    part = half // 2
    lower = ((row >= part) & (row < half)) | (row >= half + part)
    lane = jnp.where(lower, lane - 2 * devices, lane)
    mine = (lane == spot[0]) | (lane == spot[0] + devices)
    weights = rows[:, width:].astype(jnp.float32)
    scale = jnp.sum(jnp.where(mine, weights, 0.0), axis=1, keepdims=True)
    x = rows[:, :width]
    gate = jnp.dot(x, gate_w[...], preferred_element_type=jnp.float32)
    up = jnp.dot(x, up_w[...], preferred_element_type=jnp.float32)
    hidden = (gate / (1.0 + jnp.exp(-gate)) * up).astype(jnp.bfloat16)
    result = jnp.dot(hidden, down_w[...], preferred_element_type=jnp.float32) * scale
    own[...] = result[:half]
    other_x[...] = result[half : half + part].astype(jnp.bfloat16)
    other_y[...] = result[half + part :].astype(jnp.bfloat16)


def at_end(spot):
    return (spot[0] < CORES) | (spot[0] >= CORES * (LINE - 1))


def load_kernel(count, *refs):
    sources, held, sems = refs[:count], refs[count + 1 : -1], refs[-1]
    copies = [pltpu.make_async_copy(sources[n].at[0], held[n], sems.at[n]) for n in range(count)]
    for copy in copies:
        copy.start()
    for copy in copies:
        copy.wait()


def prepare_kernel(devices, part, starts, placed_hbm, tokens_hbm, ids_hbm, probs_hbm, after, *refs):
    outs, (placed, ids, probs, sems) = refs[: len(starts)], refs[len(starts) :]
    count, width = ids.shape[1], tokens_hbm.shape[1]
    moves = [(placed_hbm, placed), (ids_hbm, ids), (probs_hbm, probs)]
    for first, out in zip(starts, outs):
        moves.append((tokens_hbm.at[pl.ds(first, out.shape[0])], out.at[:, pl.ds(0, width)]))
    copies = [pltpu.make_async_copy(src, dst, sems.at[n]) for n, (src, dst) in enumerate(moves)]
    for copy in copies:
        copy.start()
    for copy in copies[:3]:
        copy.wait()
    slot = lax.broadcasted_iota(jnp.int32, (LANES, count), 0)
    weight = jnp.zeros((LANES, count), jnp.float32)
    for s in range(devices):
        total = jnp.zeros((1, count), jnp.float32)
        for k in range(ids.shape[0]):
            total += jnp.where(ids[k : k + 1, :] == placed[s], probs[k : k + 1, :], 0.0)
        high = total.astype(jnp.bfloat16).astype(jnp.float32)
        for base in (s, s + 2 * devices):
            weight = jnp.where(slot == base, high, jnp.where(slot == base + devices, total - high, weight))
    packed = weight.T.astype(jnp.bfloat16)
    lane = lax.broadcasted_iota(jnp.int32, (part, LANES), 1)
    for first, out in zip(starts, outs):
        if out.shape[1] > width:
            upper = packed[first : first + part, :]
            lower = packed[first + part : first + 2 * part, :]
            both = jnp.where(lane < 2 * devices, upper.astype(jnp.float32), lower.astype(jnp.float32))
            for row in range(0, out.shape[0], part):
                out[row : row + part, width:] = both.astype(jnp.bfloat16)
    for copy in copies[3:]:
        copy.wait()


def rest_kernel(devices, part, starts, gate_hbm, up_hbm, *refs):
    given, refs = refs[:5], refs[5:]
    outs, (gate_w, up_w), scratch, load_sems = refs[: len(starts)], refs[len(starts) : -5], refs[-5:-1], refs[-1]
    copies = [
        pltpu.make_async_copy(gate_hbm.at[0], gate_w, load_sems.at[0]),
        pltpu.make_async_copy(up_hbm.at[0], up_w, load_sems.at[1]),
    ]
    for copy in copies:
        copy.start()
    prepare_kernel(devices, part, starts, *given, *outs, *scratch)
    for copy in copies:
        copy.wait()


def gate_kernel(before, out):
    out[...] = before[...]


def join_kernel(spot, outer_x, outer_y, inner_x, inner_y, gate, out):
    part, width = outer_y.shape

    def put(upper, lower):
        out[:part] = upper[...]
        out[part:, :width] = lower[...]
        out[part:, width:] = upper[:, width:]

    @pl.when(at_end(spot))
    def _():
        put(outer_x, outer_y)

    @pl.when(jnp.logical_not(at_end(spot)))
    def _():
        put(inner_x, inner_y)


def over_kernel(start, spot, own, back, passed, out):
    part, width = out.shape[0], own.shape[1]

    @pl.when(at_end(spot))
    def _():
        total = own[start : start + part] + back[...].astype(jnp.float32)
        out[:, :width] = total.astype(out.dtype)
        if out.shape[1] > width:
            out[:, width:] = jnp.zeros((part, out.shape[1] - width), out.dtype)

    @pl.when(jnp.logical_not(at_end(spot)))
    def _():
        out[...] = passed[...]


def pass_kernel(spot, mine, passed, out):
    @pl.when(at_end(spot))
    def _():
        out[...] = mine[...]

    @pl.when(jnp.logical_not(at_end(spot)))
    def _():
        out[...] = passed[...]


def add_kernel(start, spot, own, back, other, out):
    part, width = out.shape
    total = own[start : start + part] + back[...].astype(jnp.float32)
    out[...] = (total + other[:, :width].astype(jnp.float32)).astype(out.dtype)


def ends_kernel(start, spot, outer_own, outer_back, inner_own, inner_back, other, out):
    part = out.shape[0]

    @pl.when(at_end(spot))
    def _():
        total = outer_own[start : start + part] + outer_back[...].astype(jnp.float32)
        out[...] = total.astype(out.dtype)

    @pl.when(jnp.logical_not(at_end(spot)))
    def _():
        total = inner_own[start : start + part] + inner_back[...].astype(jnp.float32)
        out[...] = (total + other[...].astype(jnp.float32)).astype(out.dtype)


def finish_kernel(first, start, parts, spot, own, *refs):
    backs, refs, (out, total, sem) = refs[:parts], refs[parts:-3], refs[-3:]
    part, width = refs[0].shape
    for n in range(parts):
        sums, near, far = refs[3 * n : 3 * n + 3]
        rows = slice(n * part, (n + 1) * part)
        mine = slice(start + n * part, start + (n + 1) * part)
        share = own[mine] + backs[n][...].astype(jnp.float32)

        @pl.when(at_end(spot))
        def _():
            total[rows] = (share + sums[...].astype(jnp.float32)).astype(out.dtype)

        @pl.when(jnp.logical_not(at_end(spot)))
        def _():
            both = near[:, :width].astype(jnp.float32) + far[...].astype(jnp.float32)
            total[rows] = (share + both).astype(out.dtype)

    copy = pltpu.make_async_copy(total, out.at[pl.ds(first, parts * part)], sem)
    copy.start()
    copy.wait()


def line_body(tokens, expert_ids, gate_probs, placed, w_gate, w_up, w_down):
    tok_rows, width = tokens.shape
    devices = lax.axis_size("exp")
    here = lax.axis_index("exp")
    last = devices // CORES - 1
    half = tok_rows // 2
    part = half // 2
    spot = here.reshape(1).astype(jnp.int32)
    vmem = pl.BlockSpec(memory_space=pltpu.VMEM)
    smem = pl.BlockSpec(memory_space=pltpu.SMEM)

    def small(kernel, shape, *operands, extra=()):
        return pl.pallas_call(
            kernel,
            in_specs=[smem] + [vmem] * (len(operands) + len(extra)),
            out_specs=vmem,
            out_shape=jax.ShapeDtypeStruct(shape, jnp.bfloat16),
            cost_estimate=pl.CostEstimate(flops=shape[0] * shape[1] * 100, bytes_accessed=0, transcendentals=0),
            compiler_params=pltpu.CompilerParams(vmem_limit_bytes=8 << 20),
        )(spot, *operands, *extra)

    def spread(pairs):
        return [(CORES * a + c, CORES * b + c) for a, b in pairs for c in range(CORES)]

    pair = spread([(0, 1), (1, 0), (last - 1, last), (last, last - 1)])
    twins = [(i, i ^ 1) for i in range(devices)]
    ends = (0, 1, devices - 2, devices - 1)
    middle = spread([(1, 2), (2, 1)]) + [(i, i ^ 1) for i in ends]

    def send(value, perm):
        return lax.ppermute(value, "exp", perm)

    long = width + LANES
    given = [pltpu.with_memory_space_constraint(v, pltpu.HBM) for v in (placed, tokens, expert_ids.T, gate_probs.T)]

    def prepare(pieces, after, *weights):
        starts = [first for first, _, _ in pieces]
        kernel = rest_kernel if weights else prepare_kernel
        loaded = [pltpu.VMEM(w.shape[1:], w.dtype) for w in weights]
        sources = [pltpu.with_memory_space_constraint(w, pltpu.HBM) for w in weights]
        return pl.pallas_call(
            functools.partial(kernel, devices, part, starts),
            in_specs=[pl.BlockSpec(memory_space=pltpu.HBM)] * (4 + len(weights)) + [pl.BlockSpec(memory_space=pl.ANY)],
            out_specs=[vmem] * (len(pieces) + len(weights)),
            out_shape=[jax.ShapeDtypeStruct(shape, jnp.bfloat16) for _, *shape in pieces] + loaded,
            scratch_shapes=[pltpu.SMEM(placed.shape, placed.dtype)]
            + [pltpu.VMEM(v.shape, v.dtype) for v in given[2:]]
            + [pltpu.SemaphoreType.DMA((3 + len(pieces),))]
            + [pltpu.SemaphoreType.DMA((2,))] * bool(weights),
            cost_estimate=pl.CostEstimate(flops=w_gate.size * 400, bytes_accessed=0, transcendentals=0)
            if weights
            else None,
            compiler_params=pltpu.CompilerParams(vmem_limit_bytes=4 << 20),
        )(*sources, *given, after)

    own_a = prepare([(0, part, long), (part, part, width)], given[0])
    others = [(half, part, long), (half + part, part, width), (0, half, long), (half, half, long)]
    made = prepare(others, own_a[0], w_gate, w_up)
    own_b, own_whole, held = made[:2], made[2:4], list(made[4:])

    hbm = pl.BlockSpec(memory_space=pltpu.HBM)

    def load(sources, after):
        count = len(sources)
        return pl.pallas_call(
            functools.partial(load_kernel, count),
            in_specs=[hbm] * count + [pl.BlockSpec(memory_space=pl.ANY)],
            out_specs=[vmem] * count,
            out_shape=[pltpu.VMEM(w.shape[1:], w.dtype) for w in sources],
            scratch_shapes=[pltpu.SemaphoreType.DMA((count,))],
            cost_estimate=pl.CostEstimate(
                flops=count * sources[0].size * 200, bytes_accessed=0, transcendentals=0
            ),
            compiler_params=pltpu.CompilerParams(vmem_limit_bytes=1 << 20),
        )(*[pltpu.with_memory_space_constraint(w, pltpu.HBM) for w in sources], after)

    held += load((w_down,), own_a[0])

    def run(block):
        count = block.shape[0]
        twin = send(block, twins)
        call = pl.pallas_call(
            functools.partial(run_kernel, width, devices),
            in_specs=[smem] + [vmem] * 5,
            out_specs=[vmem] * 3,
            out_shape=[jax.ShapeDtypeStruct((count, width), jnp.float32)]
            + [jax.ShapeDtypeStruct((part, width), jnp.bfloat16)] * 2,
            scratch_shapes=[pltpu.VMEM((2 * count, long), jnp.bfloat16)],
            cost_estimate=pl.CostEstimate(
                flops=count * width * w_gate.shape[2] * 3, bytes_accessed=0, transcendentals=0
            ),
            compiler_params=pltpu.CompilerParams(vmem_limit_bytes=count * (160 << 10)),
        )
        mine, other_x, other_y = call(spot, block, twin, *held)
        return mine, send(other_x, twins), send(other_y, twins)

    g = [[None, None] for _ in range(8)]
    m = [[None, None] for _ in range(8)]
    near_a = mid_a = far_a = far_b = mid_b = near_b = None

    def start(slot, n):
        first = n * part

        def over(sums, passed):
            return small(functools.partial(over_kernel, first), passed.shape, sums[0], sums[1 + n], passed)

        def between(sums, other):
            return small(functools.partial(add_kernel, first), (part, width), sums[0], sums[1 + n], other)

        def ends(outer_sums, inner_sums, other):
            kernel = functools.partial(ends_kernel, first)
            sums = (outer_sums[0], outer_sums[1 + n], inner_sums[0], inner_sums[1 + n])
            return small(kernel, (part, width), *sums, other)

        if slot == 0:
            pair_rows, middle_rows = own_a[n], own_a[n]
        elif slot == 1:
            pair_rows = small(pass_kernel, own_b[n].shape, own_b[n], m[0][n])
            middle_rows = g[0][n]
        elif slot == 2:
            pair_rows, middle_rows = over(near_a, m[1][n]), g[1][n]
        elif slot == 3:
            pair_rows, middle_rows = over(mid_a, m[2][n]), own_b[n]
        elif slot == 4:
            pair_rows, middle_rows = over(far_a, m[3][n]), between(mid_a, g[3][n])
        elif slot == 5:
            pair_rows, middle_rows = over(far_b, own_b[n]), between(far_a, g[4][n])
        elif slot == 6:
            pair_rows, middle_rows = ends(mid_b, near_a, m[5][n]), between(far_b, g[5][n])
        else:
            pair_rows, middle_rows = ends(near_b, near_b, m[6][n]), between(mid_b, g[6][n])
        g[slot][n] = send(pair_rows, pair)
        m[slot][n] = send(middle_rows, middle)

    def after(slot, n, result):
        g[slot][n], m[slot][n], mine = lax.optimization_barrier((g[slot][n], m[slot][n], result[:1]))
        return mine + result[1:]

    def block(outer_rows, inner_rows):
        return small(join_kernel, (half, long), *outer_rows, *inner_rows, extra=(gates[-1],))

    gates = [jnp.zeros((8, LANES), jnp.int32)]

    def gate():
        call = pl.pallas_call(
            gate_kernel,
            in_specs=[vmem],
            out_specs=vmem,
            out_shape=jax.ShapeDtypeStruct((8, LANES), jnp.int32),
            compiler_params=pltpu.CompilerParams(vmem_limit_bytes=1 << 20),
        )
        gates.append(call(gates[-1]))

    start(0, 0)
    start(0, 1)
    here_a = run(own_whole[0])
    after(0, 0, ())
    start(1, 0)
    gate()
    start(1, 1)
    near_a = after(1, 0, run(block(g[0], g[0])))
    start(2, 0)
    gate()
    start(2, 1)
    mid_a = after(2, 0, run(block(g[1], m[0])))
    start(3, 0)
    gate()
    start(3, 1)
    far_a = after(3, 0, run(block(g[2], m[1])))
    start(4, 0)
    gate()
    start(4, 1)
    far_b = after(4, 0, run(block(g[3], m[2])))
    start(5, 0)
    gate()
    start(5, 1)
    mid_b = after(5, 0, run(block(g[4], m[3])))
    start(6, 0)
    gate()
    start(6, 1)
    near_b = after(6, 0, run(block(g[5], g[1])))
    start(7, 0)
    gate()
    start(7, 1)
    here_b = run(own_whole[1])

    def finish(first, sums, ends, *extra):
        operands = (*sums, *(v for triple in ends for v in triple))
        parts = len(ends)
        return pl.pallas_call(
            functools.partial(finish_kernel, first, first % half, parts),
            in_specs=[smem] + [vmem] * len(operands) + [pl.BlockSpec(memory_space=pl.ANY)] * len(extra),
            out_specs=hbm,
            out_shape=jax.ShapeDtypeStruct((tok_rows, width), jnp.bfloat16),
            scratch_shapes=[pltpu.VMEM((parts * part, width), jnp.bfloat16), pltpu.SemaphoreType.DMA],
            input_output_aliases={len(operands) + 1: 0} if first else {},
            compiler_params=pltpu.CompilerParams(vmem_limit_bytes=8 << 20),
        )(spot, *operands, *extra)

    rows = finish(0, here_a, [(g[6][n], g[2][n], m[4][n]) for n in range(2)], gates[-1])
    rows = finish(half, here_b[:2], [(g[7][0], g[7][0], m[7][0])], rows)
    return finish(half + part, here_b[::2], [(g[7][1], g[7][1], m[7][1])], rows)


def body(tokens, *rest):
    if lax.axis_size("exp") == CORES * LINE:
        return line_body(tokens, *rest)
    return sparse_body(tokens, *rest)


def solution(mesh):
    return jax.shard_map(
        body,
        mesh=mesh,
        in_specs=(
            P(("rep", "exp"), None),
            P(("rep", "exp"), None),
            P(("rep", "exp"), None),
            P(),
            P("exp", None, None),
            P("exp", None, None),
            P("exp", None, None),
        ),
        out_specs=P(("rep", "exp"), None),
        check_vma=False,
    )
```
